32 devices in a mesh: groups: 2 (over y), ep: 4 (over z), tp: 4 (over x, core).
Axes of the slice: x: 2, y: 2, z: 4, core: 2. Of those that a mesh axis runs over, the one named last changes fastest.
Arguments:
- tokens: bfloat16 [1024, 2560], P(('groups', 'ep')), parts along dimension 0, may hold values from -6 to 6
- device_choice: int32 [1024, 3], P(('groups', 'ep')), parts along dimension 0, may hold values from 0 to 3, as said below
- local_expert: int32 [1024, 6], P(('groups', 'ep')), parts along dimension 0, may hold values from 0 to 1, as said below
- route_weight: float32 [1024, 6], P(('groups', 'ep')), parts along dimension 0, may hold values from 0.1 to 1
- prefill_ranks: int32 [4], P('groups'), parts along dimension 0, may hold values from 0 to 3, as said below
- w_gate: bfloat16 [8, 1024, 2560], P('ep', 'tp'), may hold values from -0.125 to 0.125
- w_up: bfloat16 [8, 1024, 2560], P('ep', 'tp'), may hold values from -0.125 to 0.125
- w_down: bfloat16 [8, 1024, 2560], P('ep', 'tp'), may hold values from -0.1875 to 0.1875
Outputs:
- moe_out: bfloat16 [1024, 2560], P(('groups', 'ep', 'tp')), parts along dimension 0
The draws below stay inside these ranges and needn't reach their ends.
There are 2 independent parts, one for each index of `groups`. The reference program is written for one: setup_inputs(seed, part) draws one part's arguments, and reference() takes and returns one part's arrays. A program takes and returns all parts, laid end to end along the dimension named above; an argument that names none is the same for every part. Nothing has to cross between parts.
Inputs may be any that keep to these rules, and one draw needn't show every extreme that they name: `device_choice`: each row names 3 different ranks. The rows of one rank (aligned blocks of 128 rows) name any one rank at most 96 times, and every block names some rank exactly 96 times. `local_expert`: picks 2k and 2k + 1 of a row are two different experts of the rank in column k of device_choice. So the rows of one rank choose one expert at most 96 times, and some expert is chosen exactly 96 times by the rows of every rank. `prefill_ranks`: 2 different ranks.
All inputs are finite; a program needn't handle non-finite values.
Results may differ from the reference program's by a relative error of at most 0.014.
Values may be sent and summed in bfloat16 or wider, within the bound.
A program may use at most 128 MiB of HBM per device.

```python
import math
import jax
import jax.numpy as jnp
from jax import lax

D = 2560
F = 1024
EXP_DEV = 2
TOPK = 6
DEV_TOP = 3
DEC_RANK = 8
EXPERTS = 8
RANK_ROWS = 128
PRE_RANKS = 2
ROWS = 512
CAP = 96
N_EP = 4
N_TP = 4


def route_draw(key):
    base_key = jax.random.fold_in(key, 101)
    key_star, key_local, key_order, key_rows, key_first, key_second, key_swap = jax.random.split(base_key, 7)
    star_rank = jax.random.randint(key_star, (), 0, N_EP).astype(jnp.int32)
    star_local = jax.random.randint(key_local, (), 0, EXP_DEV).astype(jnp.int32)
    others = jax.vmap(lambda one_key: jax.random.permutation(one_key, N_EP - 1))(jax.random.split(key_order, N_EP))
    rank_order = jnp.concatenate([jnp.full((N_EP, 1), star_rank, jnp.int32), (star_rank + 1 + others.astype(jnp.int32)) % N_EP], axis=1)
    row_order = jax.vmap(lambda one_key: jax.random.permutation(one_key, RANK_ROWS))(jax.random.split(key_rows, N_EP))
    cycle_pos = (DEV_TOP * row_order.astype(jnp.int32)[:, :, None] + jnp.arange(DEV_TOP, dtype=jnp.int32)[None, None, :]) % N_EP
    chosen = jnp.take_along_axis(rank_order, cycle_pos.reshape(N_EP, RANK_ROWS * DEV_TOP), axis=1)
    chosen = chosen.reshape(N_EP * RANK_ROWS, DEV_TOP).astype(jnp.int32)
    pick_shape = (N_EP * RANK_ROWS, DEV_TOP)
    first_pick = jax.random.randint(key_first, pick_shape, 0, EXP_DEV).astype(jnp.int32)
    first_pick = jnp.where(chosen == star_rank, star_local, first_pick)
    second = (first_pick + 1 + jax.random.randint(key_second, pick_shape, 0, EXP_DEV - 1).astype(jnp.int32)) % EXP_DEV
    swap_bits = jax.random.randint(key_swap, pick_shape, 0, 2)
    pick_one = jnp.where(swap_bits == 1, second, first_pick)
    pick_two = jnp.where(swap_bits == 1, first_pick, second)
    local_picks = jnp.stack([pick_one, pick_two], axis=2).reshape(N_EP * RANK_ROWS, 2 * DEV_TOP)
    return (chosen, local_picks.astype(jnp.int32))


def draw_device_choice(key, part):
    chosen, local_picks = route_draw(key)
    return chosen


def draw_local_expert(key, part):
    chosen, local_picks = route_draw(key)
    return local_picks


def draw_prefill_ranks(key, part):
    shuffled = jax.random.permutation(jax.random.fold_in(key, 211), N_EP)
    return shuffled[:PRE_RANKS].astype(jnp.int32)


def block_scale(rng, shape, shards, low, top_value):
    def one(axis_at, parts):
        steps = jax.random.uniform(jax.random.fold_in(jax.random.fold_in(rng, 6), axis_at), (parts,), jnp.float32, low / len(shards), top_value / len(shards))
        return jnp.repeat(jnp.exp(steps), shape[axis_at] // parts).reshape((-1,) + (1,) * (len(shape) - axis_at - 1))

    gain = one(*shards[0])
    for cut in shards[1:]:
        gain = gain * one(*cut)
    return gain


def centred(rng, extent, scale, limit, cuts=(), kind=jnp.bfloat16):
    level = block_scale(rng, extent, cuts, -0.22, 0.18) if cuts else 1.0
    values = jax.random.normal(rng, extent, jnp.float32) * scale * level
    return jnp.minimum(jnp.maximum(values, -limit), limit).astype(kind)


def setup_inputs(seed: int = 0, part: int = 0) -> dict:
    streams_of = jax.random.split(jax.random.key(seed), 9)
    part_splits = jax.random.split(jax.random.fold_in(streams_of[8], part), 9)
    return {
        "tokens": centred(part_splits[0], (ROWS, D), 1.0, 6.0, ((0, 4),)),
        "device_choice": draw_device_choice(jax.random.fold_in(jax.random.fold_in(streams_of[8], part), 71), part),
        "local_expert": draw_local_expert(jax.random.fold_in(jax.random.fold_in(streams_of[8], part), 71), part),
        "route_weight": jnp.clip(jnp.exp(math.log(1.0) - 2.3025851 * jax.random.uniform(part_splits[3], (ROWS, TOPK), jnp.float32) ** block_scale(part_splits[3], (ROWS, TOPK), ((0, 4),), -0.2, 0.2)), 0.1, 1.0),
        "prefill_ranks": draw_prefill_ranks(jax.random.fold_in(jax.random.fold_in(streams_of[8], part), 71), part),
        "w_gate": centred(streams_of[5], (EXPERTS, F, D), D ** -0.5, 0.125, ((0, 4), (1, 4))),
        "w_up": centred(streams_of[6], (EXPERTS, F, D), D ** -0.5, 0.125, ((0, 4), (1, 4))),
        "w_down": centred(streams_of[7], (EXPERTS, F, D), F ** -0.5, 0.1875, ((0, 4), (1, 4))),
    }


def reference(tokens, device_choice, local_expert, route_weight, prefill_ranks, w_gate, w_up, w_down):
    row_count = tokens.shape[0]
    row_ids = jnp.arange(row_count, dtype=jnp.int32)
    rank_of = row_ids // RANK_ROWS
    in_prefill = jnp.any(rank_of[:, None] == prefill_ranks[None, :], axis=1)
    is_live = (row_ids % RANK_ROWS < DEC_RANK) | in_prefill
    expert_id = jnp.repeat(device_choice, 2, axis=1) * EXP_DEV + local_expert
    weights = jnp.where(is_live[:, None], route_weight, jnp.zeros_like(route_weight))
    most_rows = N_EP * CAP
    group_width = F // N_TP

    def per_expert(totals, expert):
        matches = (expert_id == expert) & is_live[:, None]
        picked = jnp.any(matches, axis=1)
        chosen_weight = jnp.sum(jnp.where(matches, weights, jnp.zeros_like(weights)), axis=1)
        row_index = jnp.nonzero(picked, size=most_rows, fill_value=row_count)[0].astype(jnp.int32)
        safe_index = jnp.minimum(row_index, row_count - 1).astype(jnp.int32)
        gathered = tokens[safe_index]
        gate_w = lax.dynamic_index_in_dim(w_gate, expert, 0, keepdims=False)
        up_w = lax.dynamic_index_in_dim(w_up, expert, 0, keepdims=False)
        down_w = lax.dynamic_index_in_dim(w_down, expert, 0, keepdims=False)
        gate_act = jnp.dot(gathered, gate_w.T, preferred_element_type=jnp.float32)
        up_act = jnp.dot(gathered, up_w.T, preferred_element_type=jnp.float32)
        hidden = (jax.nn.silu(gate_act) * up_act).astype(jnp.bfloat16)
        summed = jnp.zeros((most_rows, tokens.shape[1]), jnp.float32)
        for group in range(N_TP):
            low = group * group_width
            part_sum = jnp.dot(hidden[:, low:low + group_width], down_w[low:low + group_width], preferred_element_type=jnp.float32)
            summed = summed + part_sum.astype(jnp.bfloat16).astype(jnp.float32)
        weighted = chosen_weight[safe_index][:, None] * summed
        totals = totals.at[row_index].add(weighted, mode="drop")
        return totals, None

    zeros_init = jnp.zeros((row_count, tokens.shape[1]), jnp.float32)
    totals, unused = lax.scan(per_expert, zeros_init, jnp.arange(EXPERTS, dtype=jnp.int32))
    return totals.astype(jnp.bfloat16)
```

```python
import functools

import jax
import jax.numpy as jnp
from jax import lax
from jax.experimental import pallas as pl
from jax.experimental.pallas import tpu as pltpu
from jax.sharding import PartitionSpec as P

TOPK = 6
DEV_TOP = 3
DEC_RANK = 8
LANES = 128
CORES = 2
VMEM_BYTES = 67_043_328
CHUNKS = 4
MESH = pl.DeviceIdType.MESH


def count_slots(slot_keys, is_live, bin_count):
    hits = (
        slot_keys[:, :, None] == jnp.arange(bin_count, dtype=jnp.int32)[None, None, :]
    ) & is_live[:, None, None]
    flat_hits = hits.astype(jnp.int32).reshape(-1, bin_count)
    before = jnp.cumsum(flat_hits, axis=0) - flat_hits
    return jnp.sum(before * flat_hits, axis=1).reshape(slot_keys.shape)


def by_collectives(
    tokens, device_choice, local_expert, route_weight, prefill_ranks, w_gate, w_up, w_down
):
    rank_count = lax.axis_size("ep")
    own_rank = lax.axis_index("ep")
    rank_rows = tokens.shape[0]
    model_width = tokens.shape[1]
    experts_here = w_gate.shape[0]
    capacity = (DEV_TOP * rank_rows + rank_count - 1) // rank_count
    row_ids = jnp.arange(rank_rows, dtype=jnp.int32)
    is_live = (row_ids < DEC_RANK) | jnp.any(prefill_ranks == own_rank)
    pair_rank = jnp.repeat(device_choice, 2, axis=1)
    expert_keys = pair_rank * experts_here + local_expert
    positions = count_slots(device_choice, is_live, rank_count)
    send_ids = device_choice * capacity + positions
    send_count = rank_count * capacity
    pick_index = expert_keys * capacity + jnp.repeat(positions, 2, axis=1)
    block_shape = (rank_count, 1, capacity, model_width)
    slot_ids = jnp.arange(send_count, dtype=jnp.int32)
    select = jnp.any(
        (send_ids[None, :, :] == slot_ids[:, None, None]) & is_live[None, :, None], axis=2
    ).astype(jnp.bfloat16)
    outgoing = (
        jnp.dot(select, tokens, preferred_element_type=jnp.float32)
        .astype(jnp.bfloat16)
        .reshape(block_shape)
    )
    blocks = lax.all_to_all(outgoing, "ep", split_axis=0, concat_axis=0, tiled=True)
    gate_act = jnp.einsum("scd,efd->secf", blocks[:, 0], w_gate, preferred_element_type=jnp.float32)
    up_act = jnp.einsum("scd,efd->secf", blocks[:, 0], w_up, preferred_element_type=jnp.float32)
    hidden = (jax.nn.silu(gate_act) * up_act).astype(jnp.bfloat16)
    partial_value = jnp.einsum(
        "secf,efd->secd", hidden, w_down, preferred_element_type=jnp.float32
    ).astype(jnp.bfloat16)
    returned = lax.all_to_all(partial_value, "ep", split_axis=0, concat_axis=0, tiled=True)
    back_width = returned.shape[3]
    flat_back = returned.reshape(-1, back_width)
    weights = jnp.where(is_live[:, None], route_weight, jnp.zeros_like(route_weight))
    shares = jnp.zeros((rank_rows, back_width), jnp.float32)
    for pick_slot in range(TOPK):
        picked_rows = flat_back[pick_index[:, pick_slot]].astype(jnp.float32)
        shares = shares + weights[:, pick_slot : pick_slot + 1] * picked_rows
    summed = lax.psum_scatter(shares.astype(jnp.bfloat16), "tp", scatter_dimension=0, tiled=True)
    return summed


def fused_kernel(
    pairs, cuts, chunks, tokens, choice_in, local_in, route_in, prefill_in, w_gate, w_up, w_down, out,
    raw, slot_rows, mix, gate, up, down, choice, local, route, prefill, total, half_out, half_in,
    side_out, side_in, path_out, near_in, over_in, back_out,
    load_sem, mix_near, mix_over, mix_recv, near_send, over_send, raw_recv, give_send, slot_recv,
    x_send, x_recv, c_send, c_recv, extra_give, extra_recv, extra_x, extra_xr, extra_c, extra_cr,
    half_send, half_recv, side_send, side_recv, path_send, near_recv, over_recv, back_send,
):
    ranks, piece_rows, width = raw.shape
    me = lax.axis_index("ep")
    spot = lax.axis_index("tp")
    column, core = spot // CORES, spot % CORES
    partner = column * CORES + (1 - core)
    across = (1 - column) * CORES + core
    experts, hidden_here, _ = w_gate.shape
    pieces = pairs * CORES
    rank_rows = pieces * piece_rows
    long_piece = piece_rows + DEC_RANK
    chunk_rows = piece_rows // chunks
    parts = range(len(cuts))

    upper = me >= ranks // 2
    end = (me == 0) | (me == ranks - 1)
    inner = ~end
    lead = spot == 0
    relay = (spot == CORES)

    def flip(k):
        return jnp.where(upper, k, ranks - 1 - k)

    place = flip(me)
    near = flip(jnp.where(end, 2, 3))
    over = flip(1)

    loads = [
        pltpu.make_async_copy(tokens.at[spot], raw.at[me], load_sem.at[0]),
        pltpu.make_async_copy(choice_in, choice, load_sem.at[1]),
        pltpu.make_async_copy(local_in, local, load_sem.at[2]),
        pltpu.make_async_copy(route_in, route, load_sem.at[3]),
        pltpu.make_async_copy(prefill_in, prefill, load_sem.at[4]),
        pltpu.make_async_copy(w_gate, gate, load_sem.at[5]),
        pltpu.make_async_copy(w_up, up, load_sem.at[6]),
        pltpu.make_async_copy(w_down, down, load_sem.at[7]),
    ]
    barrier = pltpu.get_barrier_semaphore()
    pl.semaphore_signal(barrier, inc=1, device_id={"ep": near}, device_id_type=MESH)
    pl.semaphore_signal(barrier, inc=1, device_id={"tp": across}, device_id_type=MESH)
    pl.semaphore_signal(barrier, inc=1, device_id={"tp": partner}, device_id_type=MESH)

    @pl.when(inner)
    def _():
        pl.semaphore_signal(barrier, inc=1, device_id={"ep": over}, device_id_type=MESH)

    for load in loads:
        load.start()
    for load in loads[1:5]:
        load.wait()

    hit = jnp.int32(0)
    for j in range(prefill.shape[0]):
        hit = hit + jnp.where(prefill[j] == me, 1, 0)
    table = (mix.shape[1], rank_rows)
    expert_ids = lax.broadcasted_iota(jnp.int32, table, 0)
    row_ids = lax.broadcasted_iota(jnp.int32, table, 1)
    by_expert = jnp.zeros(table, jnp.float32)
    for pick in range(TOPK):
        chosen = choice[pick // 2 : pick // 2 + 1, :] * experts + local[pick : pick + 1, :]
        by_expert = by_expert + jnp.where(expert_ids == chosen, route[pick : pick + 1, :], 0.0)
    mix[me] = jnp.where(row_ids < jnp.where(hit > 0, rank_rows, DEC_RANK), by_expert, 0.0)

    first = flip(prefill[0])
    second = flip(prefill[1])
    high, low = jnp.maximum(first, second), jnp.minimum(first, second)
    idle_high = jnp.where(high != 3, 3, jnp.where(low != 2, 2, 1))
    idle_low = 6 - high - low - idle_high
    live = [high, low]
    idle = [idle_high, idle_low]
    loads[0].wait()

    @pl.when(end)
    def _():
        pl.semaphore_wait(barrier, 3)

    @pl.when(inner)
    def _():
        pl.semaphore_wait(barrier, 4)

    def remote(src, dst, send, recv, target):
        return pltpu.make_async_remote_copy(
            src_ref=src, dst_ref=dst, send_sem=send, recv_sem=recv,
            device_id=target, device_id_type=MESH,
        )

    def columns(part):
        start, size = cuts[part]
        return pl.ds(start, size)

    def mix_to_near(block):
        return remote(mix.at[block], mix.at[block], mix_near.at[block], mix_recv.at[block], {"ep": near})

    def mix_to_over(block):
        return remote(mix.at[block], mix.at[block], mix_over.at[block], mix_recv.at[block], {"ep": over})

    def lines(c):
        return pl.ds(c * chunk_rows, chunk_rows)

    def to_near(block, c):
        piece = raw.at[block, lines(c)]
        return remote(piece, piece, near_send.at[c], raw_recv.at[block, c], {"ep": near})

    def to_over(block, c):
        piece = raw.at[block, lines(c)]
        return remote(piece, piece, over_send.at[block, c], raw_recv.at[block, c], {"ep": over})

    def slot_chunk(slot, holder, c):
        start = pl.multiple_of(holder * piece_rows + c * chunk_rows, chunk_rows)
        return slot_rows.at[slot, pl.ds(start, chunk_rows)]

    def slot_extra(slot):
        return slot_rows.at[slot, pl.ds(rank_rows, DEC_RANK)]

    def give(slot, c):
        piece = slot_chunk(slot, spot, c)
        return remote(piece, piece, give_send.at[slot, c], slot_recv.at[slot, c], {"ep": near})

    def give_extra(slot):
        piece = slot_extra(slot)
        return remote(piece, piece, extra_give.at[slot], extra_recv.at[slot], {"ep": near})

    def x_copy(slot, c):
        piece = slot_chunk(slot, spot, c)
        return remote(piece, piece, x_send.at[slot, c], x_recv.at[slot, c], {"tp": across})

    def x_extra(slot):
        piece = slot_extra(slot)
        return remote(piece, piece, extra_x.at[slot], extra_xr.at[slot], {"tp": across})

    def c_copy(slot, step, c):
        piece = slot_chunk(slot, across if step else spot, c)
        return remote(piece, piece, c_send.at[slot, step, c], c_recv.at[slot, step, c], {"tp": partner})

    def c_extra(slot):
        piece = slot_extra(slot)
        return remote(piece, piece, extra_c.at[slot], extra_cr.at[slot], {"tp": partner})

    def half_copy(slot, part):
        cols = columns(part)
        return remote(
            half_out.at[slot, :, :, cols], half_in.at[slot, :, :, cols],
            half_send.at[slot, part], half_recv.at[slot, part], {"tp": partner},
        )

    def either(long_here, make, act):
        @pl.when(long_here)
        def _():
            act(make(long_piece))

        @pl.when(~long_here)
        def _():
            act(make(piece_rows))

    def start(copy):
        copy.start()

    def wait_send(copy):
        copy.wait_send()

    def wait_recv(copy):
        copy.wait_recv()

    def side_copy(slot, part):
        cols = columns(part)
        return lambda rows: remote(
            side_out.at[slot, pl.ds(0, rows), cols], side_in.at[slot, pl.ds(0, rows), cols],
            side_send.at[slot, part], side_recv.at[slot, part], {"tp": across},
        )

    def inward(slot, part):
        cols = columns(part)
        return lambda rows: remote(
            path_out.at[slot, pl.ds(0, rows), cols], near_in.at[slot, pl.ds(0, rows), cols],
            path_send.at[slot, part], near_recv.at[slot, part], {"ep": near},
        )

    def crossing(slot, part):
        cols = columns(part)
        return lambda rows: remote(
            path_out.at[slot, pl.ds(0, rows), cols], over_in.at[1 - slot, pl.ds(0, rows), cols],
            path_send.at[slot, part], over_recv.at[1 - slot, part], {"ep": over},
        )

    def backward(part):
        cols = columns(part)
        return lambda rows: remote(
            back_out.at[pl.ds(0, rows), cols], near_in.at[0, pl.ds(0, rows), cols],
            back_send.at[part], near_recv.at[0, part], {"ep": near},
        )

    def choose(slot, which, get):
        candidates = (1, 2, 3) if slot == 0 else (0, 1, 2)
        value = get(flip(candidates[0]))
        for k in candidates[1:]:
            value = lax.select(which == k, get(flip(k)), value)
        return value

    def slot_arrive(slot, c):
        at = pl.multiple_of(spot * piece_rows + c * chunk_rows, chunk_rows)

        @pl.when(end)
        def _():
            give(slot, c).wait_recv()

        @pl.when(inner)
        def _():
            if slot == 0:
                to_near(flip(3), c).wait_recv()
                to_over(flip(3), c).start()
                to_over(flip(1), c).wait_recv()
            else:
                to_over(flip(0), c).wait_recv()
            slot_rows[slot, pl.ds(at, chunk_rows), :] = choose(
                slot, live[slot], lambda block: raw[block, lines(c), :]
            )
            give(slot, c).start()

        x_copy(slot, c).start()
        c_copy(slot, 0, c).start()
        if c == 0:
            @pl.when(lead)
            def _():
                @pl.when(end)
                def _():
                    give_extra(slot).wait_recv()

                @pl.when(inner)
                def _():
                    slot_rows[slot, pl.ds(rank_rows, DEC_RANK), :] = choose(
                        slot, idle[slot], lambda block: raw[block, 0:DEC_RANK, :]
                    )
                    give_extra(slot).start()

                x_extra(slot).start()
                c_extra(slot).start()

    def x_arrive(slot, c):
        x_copy(slot, c).wait_recv()
        c_copy(slot, 1, c).start()
        if c == 0:
            @pl.when(relay)
            def _():
                x_extra(slot).wait_recv()
                c_extra(slot).start()

    def all_here(slot):
        for c in range(chunks):
            for step in range(2):
                c_copy(slot, step, c).wait_recv()

        @pl.when(core == 1)
        def _():
            c_extra(slot).wait_recv()

    def mix_arrive(k):
        at_end, inside = 2 - k, (1, 3, 0)[k]
        block = flip(jnp.where(end, at_end, inside))
        mix_to_near(block).wait_recv()

        @pl.when(inner)
        def _():
            if inside == 3:
                mix_to_over(block).start()
            else:
                mix_to_near(block).start()

    def compute(slot):
        rows = slot_rows[slot]
        hidden = []
        for expert in range(experts):
            by_row = (((1,), (1,)), ((), ()))
            gate_act = lax.dot_general(rows, gate[expert], by_row, preferred_element_type=jnp.float32)
            up_act = lax.dot_general(rows, up[expert], by_row, preferred_element_type=jnp.float32)

            def weights(which):
                line = choose(slot, which, lambda block: mix[block, pl.ds(me * experts + expert, 1), :])
                return jnp.broadcast_to(line, (LANES, rank_rows)).T

            scale = jnp.concatenate([weights(live[slot]), weights(idle[slot])[0:DEC_RANK]], axis=0)
            scale = jnp.concatenate([scale] * (hidden_here // LANES), axis=1)
            act = gate_act / (1.0 + jnp.exp(-gate_act)) * up_act * scale
            hidden.append(act.astype(jnp.bfloat16))
        hidden = jnp.concatenate(hidden, axis=1)
        for part in parts:
            low_col, size = cuts[part]
            product = jnp.dot(
                hidden,
                down[:, :, low_col:low_col + size].reshape(experts * hidden_here, size),
                preferred_element_type=jnp.float32,
            )
            cols = columns(part)
            total[slot, :, 0:piece_rows, cols] = product[0:rank_rows].reshape(pieces, piece_rows, size)
            for piece in range(pieces):
                total[slot, piece, piece_rows:long_piece, cols] = product[rank_rows:]
            for col in range(pairs):
                half_out[slot, col, :, cols] = total[
                    slot, col * CORES + (1 - core), :, cols
                ].astype(jnp.bfloat16)
            half_copy(slot, part).start()

    def merge_half(slot):
        for part in parts:
            cols = columns(part)
            half_copy(slot, part).wait_recv()
            got = half_in[slot, 1 - column, :, cols].astype(jnp.float32)
            side_out[slot, :, cols] = (total[slot, across, :, cols] + got).astype(jnp.bfloat16)
            either(relay, side_copy(slot, part), start)
            got = half_in[slot, column, :, cols].astype(jnp.float32)
            total[slot, spot, :, cols] = total[slot, spot, :, cols] + got

    def merge_side(slot, part):
        cols = columns(part)
        either(lead, side_copy(slot, part), wait_recv)
        acc = total[slot, spot, :, cols] + side_in[slot, :, cols].astype(jnp.float32)
        total[slot, spot, :, cols] = acc

        @pl.when(end)
        def _():
            path_out[slot, :, cols] = acc.astype(jnp.bfloat16)
            either(lead, inward(slot, part), start)

    def pass_over(slot, part):
        cols = columns(part)

        @pl.when(inner)
        def _():
            either(lead, inward(slot, part), wait_recv)
            acc = total[slot, spot, :, cols] + near_in[slot, :, cols].astype(jnp.float32)
            path_out[slot, :, cols] = acc.astype(jnp.bfloat16)
            either(lead, crossing(slot, part), start)

    mix_to_near(me).start()

    @pl.when(end)
    def _():
        for c in range(chunks):
            to_near(me, c).start()

    @pl.when(inner)
    def _():
        mix_to_over(me).start()
        for c in range(chunks):
            to_over(me, c).start()

    for c in range(chunks):
        slot_arrive(0, c)
        if c == 0:
            mix_arrive(0)
    mix_arrive(1)
    for c in range(chunks):
        x_arrive(0, c)
        slot_arrive(1, c)
    mix_arrive(2)
    for load in loads[5:]:
        load.wait()
    all_here(0)
    compute(0)
    for c in range(chunks):
        x_arrive(1, c)
    merge_half(0)
    all_here(1)
    compute(1)
    for part in parts:
        merge_side(0, part)
    merge_half(1)
    for part in parts:
        pass_over(0, part)
    for part in parts:
        merge_side(1, part)
        pass_over(1, part)

    def finish(part, tops, lows):
        cols = columns(part)
        is_high, is_low = high == place, low == place
        zero = jnp.zeros((piece_rows, cuts[part][1]), jnp.float32)
        body = lax.select(is_high, tops[0:piece_rows], zero)
        rest = lax.select(idle_high == place, tops[piece_rows:long_piece], zero[0:DEC_RANK])
        if lows is not None:
            body = lax.select(is_low, lows[0:piece_rows], body)
            rest = lax.select(idle_low == place, lows[piece_rows:long_piece], rest)
        rest = lax.select(lead & ~is_high & ~is_low, rest, body[0:DEC_RANK])
        body = jnp.concatenate([rest, body[DEC_RANK:]], axis=0)
        out[:, cols] = body.astype(out.dtype)

    for part in parts:
        cols = columns(part)

        @pl.when(inner)
        def _():
            either(lead, crossing(1, part), wait_recv)
            crossed = over_in[0, :, cols].astype(jnp.float32)
            mine = total[0, spot, :, cols] + crossed
            back_out[:, cols] = mine.astype(jnp.bfloat16)
            either(lead, backward(part), start)
            either(lead, crossing(0, part), wait_recv)
            tops = mine + near_in[0, :, cols].astype(jnp.float32)
            lows = total[1, spot, :, cols] + near_in[1, :, cols].astype(jnp.float32)
            finish(part, tops, lows + over_in[1, :, cols].astype(jnp.float32))

    for part in parts:
        cols = columns(part)

        @pl.when(end)
        def _():
            either(lead, backward(part), wait_recv)
            finish(part, total[0, spot, :, cols] + near_in[0, :, cols].astype(jnp.float32), None)

    mix_to_near(me).wait_send()

    @pl.when(end)
    def _():
        for c in range(chunks):
            to_near(me, c).wait_send()

    @pl.when(inner)
    def _():
        mix_to_over(me).wait_send()
        mix_to_over(flip(3)).wait_send()
        for k in (1, 0):
            mix_to_near(flip(k)).wait_send()
        for c in range(chunks):
            to_over(me, c).wait_send()
            to_over(flip(3), c).wait_send()
            for slot in range(2):
                give(slot, c).wait_send()
        for part in parts:
            either(lead, backward(part), wait_send)

        @pl.when(lead)
        def _():
            for slot in range(2):
                give_extra(slot).wait_send()

    for slot in range(2):
        for c in range(chunks):
            x_copy(slot, c).wait_send()
            for step in range(2):
                c_copy(slot, step, c).wait_send()

        @pl.when(lead)
        def _():
            x_extra(slot).wait_send()

        @pl.when(core == 0)
        def _():
            c_extra(slot).wait_send()

        for part in parts:
            half_copy(slot, part).wait_send()
            either(relay, side_copy(slot, part), wait_send)
            either(lead, inward(slot, part), wait_send)


def column_cuts(width):
    unit = 512 if width % 512 == 0 else LANES
    return [(low, unit) for low in range(0, width, unit)]


def scratch_of(ranks, pairs, parts, chunks, experts, rank_rows, hidden_here, width):
    pieces = pairs * CORES
    piece_rows = rank_rows // pieces
    long_piece = piece_rows + DEC_RANK
    sub = (ranks * experts + 7) // 8 * 8
    arrays = [
        ((ranks, piece_rows, width), jnp.bfloat16),
        ((2, rank_rows + DEC_RANK, width), jnp.bfloat16),
        ((ranks, sub, rank_rows), jnp.float32),
        ((experts, hidden_here, width), jnp.bfloat16),
        ((experts, hidden_here, width), jnp.bfloat16),
        ((experts, hidden_here, width), jnp.bfloat16),
        ((DEV_TOP, rank_rows), jnp.int32),
        ((TOPK, rank_rows), jnp.int32),
        ((TOPK, rank_rows), jnp.float32),
        None,
        ((2, pieces, long_piece, width), jnp.float32),
        ((2, pairs, long_piece, width), jnp.bfloat16),
        ((2, pairs, long_piece, width), jnp.bfloat16),
        ((2, long_piece, width), jnp.bfloat16),
        ((2, long_piece, width), jnp.bfloat16),
        ((2, long_piece, width), jnp.bfloat16),
        ((2, long_piece, width), jnp.bfloat16),
        ((2, long_piece, width), jnp.bfloat16),
        ((long_piece, width), jnp.bfloat16),
    ]
    sems = [
        (8,), (ranks,), (ranks,), (ranks,),
        (chunks,), (ranks, chunks), (ranks, chunks), (2, chunks), (2, chunks),
        (2, chunks), (2, chunks), (2, 2, chunks), (2, 2, chunks),
        (2,), (2,), (2,), (2,), (2,), (2,),
        (2, parts), (2, parts), (2, parts), (2, parts), (2, parts), (2, parts), (2, parts), (parts,),
    ]
    return arrays, sems


def byte_count(arrays):
    total = 0
    for shape, kind in filter(None, arrays):
        size = jnp.dtype(kind).itemsize
        for extent in shape:
            size *= extent
        total += size
    return total


def on_device(
    tokens, device_choice, local_expert, route_weight, prefill_ranks, w_gate, w_up, w_down
):
    ranks = lax.axis_size("ep")
    spots = lax.axis_size("tp")
    rank_rows, width = tokens.shape
    experts, hidden_here, _ = w_gate.shape
    pairs = spots // CORES
    fits = False
    if (
        ranks == 4 and pairs == 2 and spots % CORES == 0 and prefill_ranks.shape[0] == 2
        and rank_rows == LANES and ranks * experts <= LANES and hidden_here % LANES == 0 and width % LANES == 0
    ):
        cuts = column_cuts(width)
        arrays, sems = scratch_of(
            ranks, pairs, len(cuts), CHUNKS, experts, rank_rows, hidden_here, width
        )
        fits = byte_count(arrays) < VMEM_BYTES * 3 // 4
    if not fits:
        return by_collectives(
            tokens, device_choice, local_expert, route_weight, prefill_ranks, w_gate, w_up, w_down
        )
    piece_rows = rank_rows // spots
    anywhere = pl.BlockSpec(memory_space=pl.ANY)
    in_vmem = pl.BlockSpec(memory_space=pltpu.VMEM)
    return pl.pallas_call(
        functools.partial(fused_kernel, pairs, cuts, CHUNKS),
        out_shape=jax.ShapeDtypeStruct((piece_rows, width), jnp.bfloat16),
        in_specs=[anywhere] * 8,
        out_specs=in_vmem,
        scratch_shapes=[pltpu.VMEM(*spec) if spec else pltpu.SMEM((2,), jnp.int32) for spec in arrays]
        + [pltpu.SemaphoreType.DMA(shape) for shape in sems],
        compiler_params=pltpu.CompilerParams(
            collective_id=0, has_side_effects=True, vmem_limit_bytes=VMEM_BYTES * 15 // 16
        ),
    )(
        tokens.reshape(spots, piece_rows, width), device_choice.T, local_expert.T,
        route_weight.T, prefill_ranks, w_gate, w_up, w_down,
    )


def solution(mesh):
    in_specs = (
        P(("groups", "ep"), None),
        P(("groups", "ep"), None),
        P(("groups", "ep"), None),
        P(("groups", "ep"), None),
        P("groups"),
        P("ep", "tp", None),
        P("ep", "tp", None),
        P("ep", "tp", None),
    )
    out_specs = P(("groups", "ep", "tp"), None)
    return jax.shard_map(
        on_device, mesh=mesh, in_specs=in_specs, out_specs=out_specs, check_vma=False
    )
```

```python
import functools

import jax
import jax.numpy as jnp
from jax import lax
from jax.experimental import pallas as pl
from jax.experimental.pallas import tpu as pltpu
from jax.sharding import PartitionSpec as P

TOPK = 6
DEV_TOP = 3
DEC_RANK = 8
LANES = 128
CORES = 2
VMEM_BYTES = 67_043_328
CHUNKS = 4
MESH = pl.DeviceIdType.MESH


def count_slots(slot_keys, is_live, bin_count):
    hits = (
        slot_keys[:, :, None] == jnp.arange(bin_count, dtype=jnp.int32)[None, None, :]
    ) & is_live[:, None, None]
    flat_hits = hits.astype(jnp.int32).reshape(-1, bin_count)
    before = jnp.cumsum(flat_hits, axis=0) - flat_hits
    return jnp.sum(before * flat_hits, axis=1).reshape(slot_keys.shape)


def by_collectives(
    tokens, device_choice, local_expert, route_weight, prefill_ranks, w_gate, w_up, w_down
):
    rank_count = lax.axis_size("ep")
    own_rank = lax.axis_index("ep")
    rank_rows = tokens.shape[0]
    model_width = tokens.shape[1]
    experts_here = w_gate.shape[0]
    capacity = (DEV_TOP * rank_rows + rank_count - 1) // rank_count
    row_ids = jnp.arange(rank_rows, dtype=jnp.int32)
    is_live = (row_ids < DEC_RANK) | jnp.any(prefill_ranks == own_rank)
    pair_rank = jnp.repeat(device_choice, 2, axis=1)
    expert_keys = pair_rank * experts_here + local_expert
    positions = count_slots(device_choice, is_live, rank_count)
    send_ids = device_choice * capacity + positions
    send_count = rank_count * capacity
    pick_index = expert_keys * capacity + jnp.repeat(positions, 2, axis=1)
    block_shape = (rank_count, 1, capacity, model_width)
    slot_ids = jnp.arange(send_count, dtype=jnp.int32)
    select = jnp.any(
        (send_ids[None, :, :] == slot_ids[:, None, None]) & is_live[None, :, None], axis=2
    ).astype(jnp.bfloat16)
    outgoing = (
        jnp.dot(select, tokens, preferred_element_type=jnp.float32)
        .astype(jnp.bfloat16)
        .reshape(block_shape)
    )
    blocks = lax.all_to_all(outgoing, "ep", split_axis=0, concat_axis=0, tiled=True)
    gate_act = jnp.einsum("scd,efd->secf", blocks[:, 0], w_gate, preferred_element_type=jnp.float32)
    up_act = jnp.einsum("scd,efd->secf", blocks[:, 0], w_up, preferred_element_type=jnp.float32)
    hidden = (jax.nn.silu(gate_act) * up_act).astype(jnp.bfloat16)
    partial_value = jnp.einsum(
        "secf,efd->secd", hidden, w_down, preferred_element_type=jnp.float32
    ).astype(jnp.bfloat16)
    returned = lax.all_to_all(partial_value, "ep", split_axis=0, concat_axis=0, tiled=True)
    back_width = returned.shape[3]
    flat_back = returned.reshape(-1, back_width)
    weights = jnp.where(is_live[:, None], route_weight, jnp.zeros_like(route_weight))
    shares = jnp.zeros((rank_rows, back_width), jnp.float32)
    for pick_slot in range(TOPK):
        picked_rows = flat_back[pick_index[:, pick_slot]].astype(jnp.float32)
        shares = shares + weights[:, pick_slot : pick_slot + 1] * picked_rows
    summed = lax.psum_scatter(shares.astype(jnp.bfloat16), "tp", scatter_dimension=0, tiled=True)
    return summed


def fused_kernel(
    pairs, cuts, chunks, tokens, choice_in, local_in, route_in, prefill_in, w_gate, w_up, w_down, out,
    raw, slot_rows, mix, gate, up, gate_t, up_t, down, choice, local, route, prefill, total, half_out, half_in,
    side_out, side_in, path_out, near_in, over_in, far_in, back_out,
    load_sem, mix_near, mix_over, mix_recv, near_send, over_send, raw_recv, give_send, slot_recv,
    x_send, x_recv, c_send, c_recv, extra_give, extra_recv, extra_x, extra_xr, extra_c, extra_cr,
    half_send, half_recv, side_send, side_recv, path_send, near_recv, over_recv, far_send, far_recv, back_send,
):
    ranks, piece_rows, width = raw.shape
    me = lax.axis_index("ep")
    spot = lax.axis_index("tp")
    column, core = spot // CORES, spot % CORES
    partner = column * CORES + (1 - core)
    across = (1 - column) * CORES + core
    experts, hidden_here, _ = w_gate.shape
    pieces = pairs * CORES
    rank_rows = pieces * piece_rows
    long_piece = piece_rows + DEC_RANK
    chunk_rows = piece_rows // chunks
    parts = range(len(cuts))

    upper = me >= ranks // 2
    end = (me == 0) | (me == ranks - 1)
    inner = ~end
    lead = spot == 0
    relay = (spot == CORES)

    def flip(k):
        return jnp.where(upper, k, ranks - 1 - k)

    place = flip(me)
    near = flip(jnp.where(end, 2, 3))
    over = flip(1)

    loads = [
        pltpu.make_async_copy(tokens.at[spot], raw.at[me], load_sem.at[0]),
        pltpu.make_async_copy(choice_in, choice, load_sem.at[1]),
        pltpu.make_async_copy(local_in, local, load_sem.at[2]),
        pltpu.make_async_copy(route_in, route, load_sem.at[3]),
        pltpu.make_async_copy(prefill_in, prefill, load_sem.at[4]),
        pltpu.make_async_copy(w_gate, gate, load_sem.at[5]),
        pltpu.make_async_copy(w_up, up, load_sem.at[6]),
        pltpu.make_async_copy(w_down, down, load_sem.at[7]),
    ]
    barrier = pltpu.get_barrier_semaphore()
    pl.semaphore_signal(barrier, inc=1, device_id={"ep": near}, device_id_type=MESH)
    pl.semaphore_signal(barrier, inc=1, device_id={"tp": across}, device_id_type=MESH)
    pl.semaphore_signal(barrier, inc=1, device_id={"tp": partner}, device_id_type=MESH)

    pl.semaphore_signal(barrier, inc=1, device_id={"ep": over}, device_id_type=MESH)

    @pl.when(inner)
    def _():
        pl.semaphore_signal(barrier, inc=1, device_id={"ep": flip(0)}, device_id_type=MESH)

    for load in loads:
        load.start()
    for load in loads[1:5]:
        load.wait()

    hit = jnp.int32(0)
    for j in range(prefill.shape[0]):
        hit = hit + jnp.where(prefill[j] == me, 1, 0)
    table = (mix.shape[1], rank_rows)
    expert_ids = lax.broadcasted_iota(jnp.int32, table, 0)
    row_ids = lax.broadcasted_iota(jnp.int32, table, 1)
    by_expert = jnp.zeros(table, jnp.float32)
    for pick in range(TOPK):
        chosen = choice[pick // 2 : pick // 2 + 1, :] * experts + local[pick : pick + 1, :]
        by_expert = by_expert + jnp.where(expert_ids == chosen, route[pick : pick + 1, :], 0.0)
    mix[me] = jnp.where(row_ids < jnp.where(hit > 0, rank_rows, DEC_RANK), by_expert, 0.0)

    first = flip(prefill[0])
    second = flip(prefill[1])
    high, low = jnp.maximum(first, second), jnp.minimum(first, second)
    idle_high = jnp.where(high != 3, 3, jnp.where(low != 2, 2, 1))
    idle_low = 6 - high - low - idle_high
    live = [high, low]
    idle = [idle_high, idle_low]
    loads[0].wait()

    @pl.when(end)
    def _():
        pl.semaphore_wait(barrier, 4)

    @pl.when(inner)
    def _():
        pl.semaphore_wait(barrier, 5)

    def remote(src, dst, send, recv, target):
        return pltpu.make_async_remote_copy(
            src_ref=src, dst_ref=dst, send_sem=send, recv_sem=recv,
            device_id=target, device_id_type=MESH,
        )

    def columns(part):
        start, size = cuts[part]
        return pl.ds(start, size)

    def mix_to_near(block):
        return remote(mix.at[block], mix.at[block], mix_near.at[block], mix_recv.at[block], {"ep": near})

    def mix_to_over(block):
        return remote(mix.at[block], mix.at[block], mix_over.at[block], mix_recv.at[block], {"ep": over})

    def lines(c):
        return pl.ds(c * chunk_rows, chunk_rows)

    def to_near(block, c):
        piece = raw.at[block, lines(c)]
        return remote(piece, piece, near_send.at[c], raw_recv.at[block, c], {"ep": near})

    def to_over(block, c):
        piece = raw.at[block, lines(c)]
        return remote(piece, piece, over_send.at[block, c], raw_recv.at[block, c], {"ep": over})

    def slot_chunk(slot, holder, c):
        start = pl.multiple_of(holder * piece_rows + c * chunk_rows, chunk_rows)
        return slot_rows.at[slot, pl.ds(start, chunk_rows)]

    def slot_extra(slot):
        return slot_rows.at[slot, pl.ds(rank_rows, DEC_RANK)]

    def give(slot, c):
        piece = slot_chunk(slot, spot, c)
        return remote(piece, piece, give_send.at[slot, c], slot_recv.at[slot, c], {"ep": near})

    def give_extra(slot):
        piece = slot_extra(slot)
        return remote(piece, piece, extra_give.at[slot], extra_recv.at[slot], {"ep": near})

    def x_copy(slot, c):
        piece = slot_chunk(slot, spot, c)
        return remote(piece, piece, x_send.at[slot, c], x_recv.at[slot, c], {"tp": across})

    def x_extra(slot):
        piece = slot_extra(slot)
        return remote(piece, piece, extra_x.at[slot], extra_xr.at[slot], {"tp": across})

    def c_copy(slot, step, c):
        piece = slot_chunk(slot, across if step else spot, c)
        return remote(piece, piece, c_send.at[slot, step, c], c_recv.at[slot, step, c], {"tp": partner})

    def c_extra(slot):
        piece = slot_extra(slot)
        return remote(piece, piece, extra_c.at[slot], extra_cr.at[slot], {"tp": partner})

    def half_copy(slot, part):
        cols = columns(part)
        return remote(
            half_out.at[slot, :, :, cols], half_in.at[slot, :, :, cols],
            half_send.at[slot, part], half_recv.at[slot, part], {"tp": partner},
        )

    def either(long_here, make, act):
        @pl.when(long_here)
        def _():
            act(make(long_piece))

        @pl.when(~long_here)
        def _():
            act(make(piece_rows))

    def start(copy):
        copy.start()

    def wait_send(copy):
        copy.wait_send()

    def wait_recv(copy):
        copy.wait_recv()

    def side_copy(slot, part):
        cols = columns(part)
        return lambda rows: remote(
            side_out.at[slot, pl.ds(0, rows), cols], side_in.at[slot, pl.ds(0, rows), cols],
            side_send.at[slot, part], side_recv.at[slot, part], {"tp": across},
        )

    def inward(slot, part):
        cols = columns(part)
        return lambda rows: remote(
            path_out.at[slot, pl.ds(0, rows), cols], near_in.at[slot, pl.ds(0, rows), cols],
            path_send.at[slot, part], near_recv.at[slot, part], {"ep": near},
        )

    def crossing(slot, part):
        cols = columns(part)
        return lambda rows: remote(
            path_out.at[slot, pl.ds(0, rows), cols], over_in.at[1 - slot, pl.ds(0, rows), cols],
            path_send.at[slot, part], over_recv.at[1 - slot, part], {"ep": over},
        )

    def direct(part):
        cols = columns(part)
        return lambda rows: remote(
            path_out.at[1, pl.ds(0, rows), cols], far_in.at[pl.ds(0, rows), cols],
            far_send.at[part], far_recv.at[part], {"ep": over},
        )

    def backward(part):
        cols = columns(part)
        return lambda rows: remote(
            back_out.at[pl.ds(0, rows), cols], near_in.at[0, pl.ds(0, rows), cols],
            back_send.at[part], near_recv.at[0, part], {"ep": near},
        )

    def choose(slot, which, get):
        candidates = (1, 2, 3) if slot == 0 else (0, 1, 2)
        value = get(flip(candidates[0]))
        for k in candidates[1:]:
            value = lax.select(which == k, get(flip(k)), value)
        return value

    def slot_arrive(slot, c):
        at = pl.multiple_of(spot * piece_rows + c * chunk_rows, chunk_rows)

        @pl.when(end)
        def _():
            give(slot, c).wait_recv()

        @pl.when(inner)
        def _():
            if slot == 0:
                to_near(flip(3), c).wait_recv()
                to_over(flip(3), c).start()
                to_over(flip(1), c).wait_recv()
            else:
                to_over(flip(0), c).wait_recv()
            slot_rows[slot, pl.ds(at, chunk_rows), :] = choose(
                slot, live[slot], lambda block: raw[block, lines(c), :]
            )
            give(slot, c).start()

        x_copy(slot, c).start()
        c_copy(slot, 0, c).start()
        if c == 0:
            @pl.when(lead)
            def _():
                @pl.when(end)
                def _():
                    give_extra(slot).wait_recv()

                @pl.when(inner)
                def _():
                    slot_rows[slot, pl.ds(rank_rows, DEC_RANK), :] = choose(
                        slot, idle[slot], lambda block: raw[block, 0:DEC_RANK, :]
                    )
                    give_extra(slot).start()

                x_extra(slot).start()
                c_extra(slot).start()

    def x_arrive(slot, c):
        x_copy(slot, c).wait_recv()
        c_copy(slot, 1, c).start()
        if c == 0:
            @pl.when(relay)
            def _():
                x_extra(slot).wait_recv()
                c_extra(slot).start()

    def all_here(slot):
        for c in range(chunks):
            for step in range(2):
                c_copy(slot, step, c).wait_recv()

        @pl.when(core == 1)
        def _():
            c_extra(slot).wait_recv()

    def mix_arrive(k):
        at_end, inside = 2 - k, (1, 3, 0)[k]
        block = flip(jnp.where(end, at_end, inside))
        mix_to_near(block).wait_recv()

        @pl.when(inner)
        def _():
            if inside == 3:
                mix_to_over(block).start()
            else:
                mix_to_near(block).start()

    def compute(slot):
        rows = slot_rows[slot]
        hidden = []
        for expert in range(experts):
            gate_act = jnp.dot(rows, gate_t[expert], preferred_element_type=jnp.float32)
            up_act = jnp.dot(rows, up_t[expert], preferred_element_type=jnp.float32)

            def weights(which):
                line = choose(slot, which, lambda block: mix[block, pl.ds(me * experts + expert, 1), :])
                return jnp.broadcast_to(line, (LANES, rank_rows)).T

            scale = jnp.concatenate([weights(live[slot]), weights(idle[slot])[0:DEC_RANK]], axis=0)
            scale = jnp.concatenate([scale] * (hidden_here // LANES), axis=1)
            act = gate_act / (1.0 + jnp.exp(-gate_act)) * up_act * scale
            hidden.append(act.astype(jnp.bfloat16))
        hidden = jnp.concatenate(hidden, axis=1)
        for part in parts:
            low_col, size = cuts[part]
            product = jnp.dot(
                hidden,
                down[:, :, low_col:low_col + size].reshape(experts * hidden_here, size),
                preferred_element_type=jnp.float32,
            )
            cols = columns(part)
            total[slot, :, 0:piece_rows, cols] = product[0:rank_rows].reshape(pieces, piece_rows, size)
            for piece in range(pieces):
                total[slot, piece, piece_rows:long_piece, cols] = product[rank_rows:]
            for col in range(pairs):
                half_out[slot, col, :, cols] = total[
                    slot, col * CORES + (1 - core), :, cols
                ].astype(jnp.bfloat16)
            half_copy(slot, part).start()

    def merge_half(slot):
        for part in parts:
            cols = columns(part)
            half_copy(slot, part).wait_recv()
            got = half_in[slot, 1 - column, :, cols].astype(jnp.float32)
            side_out[slot, :, cols] = (total[slot, across, :, cols] + got).astype(jnp.bfloat16)
            either(relay, side_copy(slot, part), start)
            got = half_in[slot, column, :, cols].astype(jnp.float32)
            total[slot, spot, :, cols] = total[slot, spot, :, cols] + got

    def merge_side(slot, part):
        cols = columns(part)
        either(lead, side_copy(slot, part), wait_recv)
        acc = total[slot, spot, :, cols] + side_in[slot, :, cols].astype(jnp.float32)
        total[slot, spot, :, cols] = acc

        if slot == 1:
            path_out[slot, :, cols] = acc.astype(jnp.bfloat16)

            @pl.when(end)
            def _():
                either(lead, direct(part), start)

            @pl.when(inner)
            def _():
                either(lead, crossing(slot, part), start)
        else:
            @pl.when(end)
            def _():
                path_out[slot, :, cols] = acc.astype(jnp.bfloat16)
                either(lead, inward(slot, part), start)

    def pass_over(slot, part):
        cols = columns(part)

        @pl.when(inner)
        def _():
            either(lead, inward(slot, part), wait_recv)
            acc = total[slot, spot, :, cols] + near_in[slot, :, cols].astype(jnp.float32)
            path_out[slot, :, cols] = acc.astype(jnp.bfloat16)
            either(lead, crossing(slot, part), start)

    mix_to_near(me).start()

    @pl.when(end)
    def _():
        for c in range(chunks):
            to_near(me, c).start()

    @pl.when(inner)
    def _():
        mix_to_over(me).start()
        for c in range(chunks):
            to_over(me, c).start()

    for load in loads[5:]:
        load.wait()
    for expert in range(experts):
        gate_t[expert] = gate[expert].T
        up_t[expert] = up[expert].T
    for c in range(chunks):
        slot_arrive(0, c)
        if c == 0:
            mix_arrive(0)
    mix_arrive(1)
    for c in range(chunks):
        x_arrive(0, c)
        slot_arrive(1, c)
    mix_arrive(2)
    all_here(0)
    compute(0)
    for c in range(chunks):
        x_arrive(1, c)
    merge_half(0)
    all_here(1)
    compute(1)
    merge_half(1)
    for part in parts:
        merge_side(0, part)
    for part in parts:
        merge_side(1, part)

    @pl.when(end)
    def _():
        for part in parts:
            either(lead, inward(1, part), start)

    for part in parts:
        pass_over(0, part)

    def finish(part, tops, lows):
        cols = columns(part)
        is_high, is_low = high == place, low == place
        zero = jnp.zeros((piece_rows, cuts[part][1]), jnp.float32)
        body = lax.select(is_high, tops[0:piece_rows], zero)
        rest = lax.select(idle_high == place, tops[piece_rows:long_piece], zero[0:DEC_RANK])
        if lows is not None:
            body = lax.select(is_low, lows[0:piece_rows], body)
            rest = lax.select(idle_low == place, lows[piece_rows:long_piece], rest)
        rest = lax.select(lead & ~is_high & ~is_low, rest, body[0:DEC_RANK])
        body = jnp.concatenate([rest, body[DEC_RANK:]], axis=0)
        out[:, cols] = body.astype(out.dtype)

    @pl.when(inner)
    def _():
        for part in parts:
            cols = columns(part)
            either(lead, crossing(1, part), wait_recv)
            either(lead, direct(part), wait_recv)
            mine = total[0, spot, :, cols] + over_in[0, :, cols].astype(jnp.float32)
            mine = mine + far_in[:, cols].astype(jnp.float32)
            back_out[:, cols] = mine.astype(jnp.bfloat16)
            either(lead, backward(part), start)
            total[0, spot, :, cols] = mine
        for part in parts:
            cols = columns(part)
            either(lead, crossing(0, part), wait_recv)
            either(lead, inward(1, part), wait_recv)
            tops = total[0, spot, :, cols] + near_in[0, :, cols].astype(jnp.float32)
            lows = total[1, spot, :, cols] + near_in[1, :, cols].astype(jnp.float32)
            finish(part, tops, lows + over_in[1, :, cols].astype(jnp.float32))

    @pl.when(end)
    def _():
        for part in parts:
            cols = columns(part)
            either(lead, backward(part), wait_recv)
            finish(part, total[0, spot, :, cols] + near_in[0, :, cols].astype(jnp.float32), None)

    mix_to_near(me).wait_send()

    @pl.when(end)
    def _():
        for c in range(chunks):
            to_near(me, c).wait_send()
        for part in parts:
            either(lead, direct(part), wait_send)

    @pl.when(inner)
    def _():
        mix_to_over(me).wait_send()
        mix_to_over(flip(3)).wait_send()
        for k in (1, 0):
            mix_to_near(flip(k)).wait_send()
        for c in range(chunks):
            to_over(me, c).wait_send()
            to_over(flip(3), c).wait_send()
            for slot in range(2):
                give(slot, c).wait_send()
        for part in parts:
            either(lead, backward(part), wait_send)

        @pl.when(lead)
        def _():
            for slot in range(2):
                give_extra(slot).wait_send()

    for slot in range(2):
        for c in range(chunks):
            x_copy(slot, c).wait_send()
            for step in range(2):
                c_copy(slot, step, c).wait_send()

        @pl.when(lead)
        def _():
            x_extra(slot).wait_send()

        @pl.when(core == 0)
        def _():
            c_extra(slot).wait_send()

        for part in parts:
            half_copy(slot, part).wait_send()
            either(relay, side_copy(slot, part), wait_send)
            either(lead, inward(slot, part), wait_send)


def column_cuts(width):
    unit = 512 if width % 512 == 0 else LANES
    return [(low, unit) for low in range(0, width, unit)]


def scratch_of(ranks, pairs, parts, chunks, experts, rank_rows, hidden_here, width):
    pieces = pairs * CORES
    piece_rows = rank_rows // pieces
    long_piece = piece_rows + DEC_RANK
    sub = (ranks * experts + 7) // 8 * 8
    arrays = [
        ((ranks, piece_rows, width), jnp.bfloat16),
        ((2, rank_rows + DEC_RANK, width), jnp.bfloat16),
        ((ranks, sub, rank_rows), jnp.float32),
        ((experts, hidden_here, width), jnp.bfloat16),
        ((experts, hidden_here, width), jnp.bfloat16),
        ((experts, width, hidden_here), jnp.bfloat16),
        ((experts, width, hidden_here), jnp.bfloat16),
        ((experts, hidden_here, width), jnp.bfloat16),
        ((DEV_TOP, rank_rows), jnp.int32),
        ((TOPK, rank_rows), jnp.int32),
        ((TOPK, rank_rows), jnp.float32),
        None,
        ((2, pieces, long_piece, width), jnp.float32),
        ((2, pairs, long_piece, width), jnp.bfloat16),
        ((2, pairs, long_piece, width), jnp.bfloat16),
        ((2, long_piece, width), jnp.bfloat16),
        ((2, long_piece, width), jnp.bfloat16),
        ((2, long_piece, width), jnp.bfloat16),
        ((2, long_piece, width), jnp.bfloat16),
        ((2, long_piece, width), jnp.bfloat16),
        ((long_piece, width), jnp.bfloat16),
        ((long_piece, width), jnp.bfloat16),
    ]
    sems = [
        (8,), (ranks,), (ranks,), (ranks,),
        (chunks,), (ranks, chunks), (ranks, chunks), (2, chunks), (2, chunks),
        (2, chunks), (2, chunks), (2, 2, chunks), (2, 2, chunks),
        (2,), (2,), (2,), (2,), (2,), (2,),
        (2, parts), (2, parts), (2, parts), (2, parts), (2, parts), (2, parts), (2, parts), (parts,), (parts,), (parts,),
    ]
    return arrays, sems


def byte_count(arrays):
    total = 0
    for shape, kind in filter(None, arrays):
        size = jnp.dtype(kind).itemsize
        for extent in shape:
            size *= extent
        total += size
    return total


def on_device(
    tokens, device_choice, local_expert, route_weight, prefill_ranks, w_gate, w_up, w_down
):
    ranks = lax.axis_size("ep")
    spots = lax.axis_size("tp")
    rank_rows, width = tokens.shape
    experts, hidden_here, _ = w_gate.shape
    pairs = spots // CORES
    fits = False
    if (
        ranks == 4 and pairs == 2 and spots % CORES == 0 and prefill_ranks.shape[0] == 2
        and rank_rows == LANES and ranks * experts <= LANES and hidden_here % LANES == 0 and width % LANES == 0
    ):
        cuts = column_cuts(width)
        arrays, sems = scratch_of(
            ranks, pairs, len(cuts), CHUNKS, experts, rank_rows, hidden_here, width
        )
        fits = byte_count(arrays) < VMEM_BYTES * 3 // 4
    if not fits:
        return by_collectives(
            tokens, device_choice, local_expert, route_weight, prefill_ranks, w_gate, w_up, w_down
        )
    piece_rows = rank_rows // spots
    anywhere = pl.BlockSpec(memory_space=pl.ANY)
    in_vmem = pl.BlockSpec(memory_space=pltpu.VMEM)
    return pl.pallas_call(
        functools.partial(fused_kernel, pairs, cuts, CHUNKS),
        out_shape=jax.ShapeDtypeStruct((piece_rows, width), jnp.bfloat16),
        in_specs=[anywhere] * 8,
        out_specs=in_vmem,
        scratch_shapes=[pltpu.VMEM(*spec) if spec else pltpu.SMEM((2,), jnp.int32) for spec in arrays]
        + [pltpu.SemaphoreType.DMA(shape) for shape in sems],
        compiler_params=pltpu.CompilerParams(
            collective_id=0, has_side_effects=True, vmem_limit_bytes=VMEM_BYTES * 15 // 16
        ),
    )(
        tokens.reshape(spots, piece_rows, width), device_choice.T, local_expert.T,
        route_weight.T, prefill_ranks, w_gate, w_up, w_down,
    )


def solution(mesh):
    in_specs = (
        P(("groups", "ep"), None),
        P(("groups", "ep"), None),
        P(("groups", "ep"), None),
        P(("groups", "ep"), None),
        P("groups"),
        P("ep", "tp", None),
        P("ep", "tp", None),
        P("ep", "tp", None),
    )
    out_specs = P(("groups", "ep", "tp"), None)
    return jax.shard_map(
        on_device, mesh=mesh, in_specs=in_specs, out_specs=out_specs, check_vma=False
    )
```
